32 devices in a mesh: batch: 4 (over y, x), feat: 8 (over z, core).
Axes of the slice: x: 2, y: 2, z: 4, core: 2. Of those that a mesh axis runs over, the one named last changes fastest.
Arguments:
- view_a: bfloat16 [1024, 8192], P('batch', 'feat'), may hold values from -16 to 16
- view_b: bfloat16 [1024, 8192], P('batch', 'feat'), may hold values from -16 to 16
Outputs:
- loss_value: float32 [], replicated
- grad_a: float32 [1024, 8192], P('batch', 'feat')
- grad_b: float32 [1024, 8192], P('batch', 'feat')
The draws below stay inside these ranges and needn't reach their ends.
All inputs are finite; a program needn't handle non-finite values.
Results may differ from the reference program's by a relative error of at most 0.0026.
Values may be sent and summed in bfloat16 or wider, within the bound.
No kernel may reach another device: no remote copies, remote signals or barrier semaphores. Data moves between devices by JAX's collectives and lax.ppermute only.
A program may use at most 64 MiB of HBM per device.

```python
import math
import jax
import jax.numpy as jnp
from jax import lax

F = 8192
BATCH = 1024


def common_signal(key):
    base = jax.random.normal(jax.random.fold_in(key, 102), (BATCH, F), jnp.float32)
    factors = jax.random.normal(jax.random.fold_in(key, 103), (BATCH, 32), jnp.float32)
    loadings = 0.25 * jax.random.normal(jax.random.fold_in(key, 104), (32, F), jnp.float32)
    return base + jnp.dot(factors, loadings, precision=lax.Precision.HIGHEST)


def shaped_view(key, salt):
    common = common_signal(key)
    noise = jax.random.normal(jax.random.fold_in(key, salt), (BATCH, F), jnp.float32)
    spread = math.log(2.0)
    factor = jnp.exp(jax.random.uniform(jax.random.fold_in(key, salt + 1), (F,), jnp.float32, -spread, spread))
    offset = jax.random.uniform(jax.random.fold_in(key, salt + 2), (F,), jnp.float32, -2.0, 2.0)
    drift = jax.random.uniform(jax.random.fold_in(key, salt + 3), (F,), jnp.float32, -1.0, 1.0)
    ramp = 2.0 * (jnp.arange(BATCH, dtype=jnp.float32) + 0.5) / BATCH - 1.0
    values = (common + 0.8 * noise) * factor + offset + drift * ramp[:, None]
    return jnp.clip(values, -16.0, 16.0).astype(jnp.bfloat16)


def draw_view_a(key, part):
    return shaped_view(key, 201)


def draw_view_b(key, part):
    return shaped_view(key, 301)


def setup_inputs(seed: int = 0) -> dict:
    streams_of = jax.random.split(jax.random.key(seed), 3)
    return {
        "view_a": draw_view_a(jax.random.fold_in(streams_of[2], 71), 0),
        "view_b": draw_view_b(jax.random.fold_in(streams_of[2], 71), 0),
    }


variance_floor = 0.25
redundancy = 0.0051

def normalize(view):
    values = view.astype(jnp.float32)
    center = lax.optimization_barrier(jnp.mean(values, axis=0))
    shifted = values - center
    variance = lax.optimization_barrier(jnp.mean(shifted * shifted, axis=0))
    factor = lax.rsqrt(variance + variance_floor)
    return (shifted * factor, factor)

def backward(dnorm, normed, factor):
    first = lax.optimization_barrier(jnp.mean(dnorm, axis=0))
    second = lax.optimization_barrier(jnp.mean(dnorm * normed, axis=0))
    return (dnorm - first - normed * second) * factor

def reference(view_a, view_b):
    normed_a, factor_a = normalize(view_a)
    normed_b, factor_b = normalize(view_b)
    low_a = normed_a.astype(jnp.bfloat16)
    low_b = normed_b.astype(jnp.bfloat16)
    batch_total, feature_total = view_a.shape
    block_cols = math.gcd(feature_total, 1024)
    blocks = feature_total // block_cols
    stacked_b = low_b.reshape(batch_total, blocks, block_cols).transpose(1, 0, 2)
    row_ids = jnp.arange(feature_total, dtype=jnp.int32)

    def advance(carry, inputs):
        grad_acc, loss_acc = carry
        part_b, number = inputs
        cross_block = lax.dot_general(low_a, part_b, (((0,), (0,)), ((), ())), preferred_element_type=jnp.float32) / batch_total
        col_ids = number * block_cols + jnp.arange(block_cols, dtype=jnp.int32)
        diagonal_mask = row_ids[:, None] == col_ids[None, :]
        missing = 1.0 - cross_block
        loss_acc = loss_acc + jnp.sum(jnp.where(diagonal_mask, missing * missing, redundancy * cross_block * cross_block))
        dcross = jnp.where(diagonal_mask, 2.0 * (cross_block - 1.0), 2.0 * redundancy * cross_block).astype(jnp.bfloat16)
        dnorm_part = jnp.dot(low_a, dcross, preferred_element_type=jnp.float32)
        grad_acc = grad_acc + lax.dot_general(part_b, dcross, (((1,), (1,)), ((), ())), preferred_element_type=jnp.float32)
        return ((grad_acc, loss_acc), dnorm_part)
    start = (jnp.zeros((batch_total, feature_total), jnp.float32), jnp.zeros((), jnp.float32))
    (dnorm_a, loss_sum), pieces = lax.scan(advance, start, (stacked_b, jnp.arange(blocks, dtype=jnp.int32)))
    dnorm_b = pieces.transpose(1, 0, 2).reshape(batch_total, feature_total)
    grad_a = backward(dnorm_a, normed_a, factor_a)
    grad_b = backward(dnorm_b, normed_b, factor_b)
    return (loss_sum / feature_total, grad_a, grad_b)
```

```python
import jax
import jax.numpy as jnp
from jax import lax
from jax.sharding import PartitionSpec as P

variance_floor = 0.25
redundancy = 0.0051


def power_of_two(n):
    return n & (n - 1) == 0


def xor_send(x, axis, k):
    n = lax.axis_size(axis)
    return lax.ppermute(x, axis, [(i, i ^ k) for i in range(n)])


def shift_send(x, axis, pairs):
    return lax.ppermute(x, axis, pairs)


def gather_rows(x):
    n = lax.axis_size("batch")
    if n == 4:
        half = x.shape[0] // 2
        near_x = xor_send(x, "batch", 1)
        near_y = xor_send(x, "batch", 2)
        far_low = xor_send(near_x[:half], "batch", 2)
        far_high = xor_send(near_y[half:], "batch", 1)
        return [x, near_x, near_y, jnp.concatenate([far_low, far_high], axis=0)]
    return [x] + [
        lax.ppermute(x, "batch", [((i + k) % n, i) for i in range(n)]) for k in range(1, n)
    ]


def butterfly(x, axis):
    n = lax.axis_size(axis)
    if not power_of_two(n):
        return lax.psum(x, axis)
    parts = [x] + [xor_send(x, axis, k) for k in range(1, n)]
    while len(parts) > 1:
        parts = [parts[i] + parts[i + 1] for i in range(0, len(parts), 2)]
    return parts[0]


def reduce_gram(part):
    n = lax.axis_size("feat")
    lines = n // 2
    index = lax.axis_index("feat")
    core = index % 2
    line = index // 2
    rows, width = part.shape
    halves = part.reshape(2, rows // 2, width)
    mine = lax.dynamic_index_in_dim(halves, core, 0, keepdims=False)
    other = lax.dynamic_index_in_dim(halves, 1 - core, 0, keepdims=False)
    chip = mine + xor_send(other, "feat", 1)
    blocks = chip.reshape(lines, rows // n, width)
    total = lax.dynamic_index_in_dim(blocks, line, 0, keepdims=False)
    low_blocks = blocks.astype(jnp.bfloat16)
    for k in range(1, lines):
        sent = lax.dynamic_index_in_dim(low_blocks, (line + k) % lines, 0, keepdims=False)
        pairs = [(i, (i + 2 * k) % n) for i in range(n)]
        total = total + lax.ppermute(sent, "feat", pairs).astype(jnp.float32)
    low = total.astype(jnp.bfloat16)
    stacked = [low]
    for k in range(1, lines):
        pairs = [((i + 2 * k) % n, i) for i in range(n)]
        stacked.append(lax.ppermute(low, "feat", pairs))
    ring = jnp.concatenate(stacked + stacked, axis=0)
    step = rows // n
    half = lax.dynamic_slice_in_dim(ring, (lines - line) % lines * step, lines * step, 0)
    peer = xor_send(half, "feat", 1)
    first = jnp.where(core == 0, half, peer)
    second = jnp.where(core == 0, peer, half)
    return jnp.concatenate([first, second], axis=0)


def normalize(pieces, batch_total):
    values = [p.astype(jnp.float32) for p in pieces]
    mean = sum(jnp.sum(v, axis=0) for v in values) / batch_total
    var = sum(jnp.sum((v - mean) ** 2, axis=0) for v in values) / batch_total
    factor = lax.rsqrt(var + variance_floor)
    low = jnp.concatenate([((v - mean) * factor).astype(jnp.bfloat16) for v in values], axis=0)
    return (values[0] - mean) * factor, factor, low


def gram(low, rows):
    return lax.dot_general(
        low[:rows], low, (((1,), (1,)), ((), ())), preferred_element_type=jnp.float32
    )


def local(view_a, view_b):
    rows, cols = view_a.shape
    batch_size = lax.axis_size("batch")
    batch_total = rows * batch_size
    feature_total = cols * lax.axis_size("feat")
    pieces_a = gather_rows(view_a)
    pieces_b = gather_rows(view_b)
    normed_a, factor_a, low_a = normalize(pieces_a, batch_total)
    gram_a = reduce_gram(gram(low_a, rows))
    normed_b, factor_b, low_b = normalize(pieces_b, batch_total)
    gram_b = reduce_gram(gram(low_b, rows))
    diag = (
        jnp.sum(low_a.astype(jnp.float32) * low_b.astype(jnp.float32), axis=0) / batch_total
    )
    diag_loss = butterfly(
        jnp.sum((1.0 - diag) ** 2 - redundancy * diag * diag).reshape(1, 1), "feat"
    )
    pull = 2.0 * (diag - 1.0) - 2.0 * redundancy * diag
    scale = 2.0 * redundancy / batch_total
    dnorm_b = (
        jnp.dot(gram_a, low_b, preferred_element_type=jnp.float32) * scale
        + low_a[:rows].astype(jnp.float32) * pull
    )
    dnorm_a = (
        jnp.dot(gram_b, low_a, preferred_element_type=jnp.float32) * scale
        + low_b[:rows].astype(jnp.float32) * pull
    )
    spread = jnp.sum(gram_a.astype(jnp.float32) * gram_b.astype(jnp.float32))
    loss_part = (
        diag_loss[0, 0] / batch_size + redundancy * (spread / (batch_total * batch_total))
    )
    stats = jnp.stack(
        [
            jnp.sum(dnorm_a, axis=0),
            jnp.sum(dnorm_a * normed_a, axis=0),
            jnp.sum(dnorm_b, axis=0),
            jnp.sum(dnorm_b * normed_b, axis=0),
            jnp.full((cols,), loss_part),
        ]
    )
    totals = butterfly(stats, "batch")
    loss_value = totals[4, 0] / feature_total
    means = totals[:4] / batch_total
    grad_a = (dnorm_a - means[0] - normed_a * means[1]) * factor_a
    grad_b = (dnorm_b - means[2] - normed_b * means[3]) * factor_b
    return (loss_value, grad_a, grad_b)


def solution(mesh):
    return jax.shard_map(
        local,
        mesh=mesh,
        in_specs=(P("batch", "feat"), P("batch", "feat")),
        out_specs=(P(), P("batch", "feat"), P("batch", "feat")),
        check_vma=False,
    )
```

```python
import jax
import jax.numpy as jnp
from jax import lax
from jax.experimental import pallas as pl
from jax.experimental.pallas import tpu as pltpu
from jax.sharding import PartitionSpec as P


variance_floor = 0.25
redundancy = 0.0051


def xor_send(x, axis, k):
    n = lax.axis_size(axis)
    return lax.ppermute(x, axis, [(i, i ^ k) for i in range(n)])


def gather_near(x):
    return [x, xor_send(x, "batch", 1), xor_send(x, "batch", 2)]


def gather_far(pieces):
    own, near_x, near_y = pieces
    half = own.shape[0] // 2
    far_low = xor_send(near_x[:half], "batch", 2)
    far_high = xor_send(near_y[half:], "batch", 1)
    return [own, near_x, near_y, jnp.concatenate([far_low, far_high], axis=0)]


def tree(parts):
    while len(parts) > 1:
        parts = [parts[i] + parts[i + 1] for i in range(0, len(parts), 2)]
    return parts[0]


def batch_sum(x):
    n = lax.axis_size("batch")
    return tree([x] + [xor_send(x, "batch", k) for k in range(1, n)])


def scatter_gram(part):
    n = lax.axis_size("feat")
    lines = n // 2
    index = lax.axis_index("feat")
    core = index % 2
    line = index // 2
    rows, width = part.shape
    halves = part.reshape(2, rows // 2, width)
    mine = lax.dynamic_index_in_dim(halves, core, 0, keepdims=False)
    other = lax.dynamic_index_in_dim(halves, 1 - core, 0, keepdims=False)
    other = xor_send(other, "feat", 1)
    blocks = (mine + other).reshape(lines, rows // n, width)
    terms = [lax.dynamic_index_in_dim(blocks, line, 0, keepdims=False)]
    low_blocks = blocks.astype(jnp.bfloat16)
    for k in range(1, lines):
        sent = lax.dynamic_index_in_dim(low_blocks, line ^ k, 0, keepdims=False)
        terms.append(xor_send(sent, "feat", 2 * k))
    return terms


def add_terms(terms):
    return sum(t.astype(jnp.float32) for t in terms[1:]) + terms[0]


def own_loss(terms, own_a, diag, batch_size, batch_total):
    rows, width = terms[0].shape

    def body(*refs):
        *term_refs, own_ref, diag_ref, out = refs
        total = add_terms([t[...] for t in term_refs])
        d = diag_ref[...]
        ends = jnp.sum((1.0 - d) ** 2 - redundancy * d * d, keepdims=True)
        spread = jnp.sum(total * own_ref[...], keepdims=True)
        value = ends / batch_size + redundancy * (spread / (batch_total * batch_total))
        value = jnp.broadcast_to(value, (rows, 128))
        high = value.astype(jnp.bfloat16).astype(jnp.float32)
        rest = value - high
        mid = rest.astype(jnp.bfloat16).astype(jnp.float32)
        column = lax.broadcasted_iota(jnp.int32, (rows, 128), 1)
        tail = jnp.where(
            column == 0, high, jnp.where(column == 1, mid, jnp.where(column == 2, rest - mid, 0.0))
        )
        out[:, :width] = total.astype(jnp.bfloat16)
        out[:, width:] = tail.astype(jnp.bfloat16)

    return pl.pallas_call(
        body,
        out_shape=jax.ShapeDtypeStruct((rows, width + 128), jnp.bfloat16),
        compiler_params=pltpu.CompilerParams(vmem_limit_bytes=4 * 1024 * 1024),
        name="own_loss",
    )(*terms, own_a, diag)


def spread_rows(sent):
    lines = lax.axis_size("feat") // 2
    parts = [sent] + [xor_send(sent, "feat", 2 * k) for k in range(1, lines)]
    half = jnp.concatenate(parts, axis=0)
    return half, xor_send(half, "feat", 1)


def assemble(half, peer, width):
    lines = lax.axis_size("feat") // 2
    index = lax.axis_index("feat").reshape(1)
    step = half.shape[0] // lines
    beside = half.shape[1] > width

    def body(index_ref, half_ref, peer_ref, out, *rest):
        core = index_ref[0] % 2
        line = index_ref[0] // 2
        for ref, side in ((half_ref, core), (peer_ref, 1 - core)):
            for k in range(lines):
                at = pl.multiple_of((side * lines + (line ^ k)) * step, step)
                out[pl.ds(at, step), :] = ref[k * step : (k + 1) * step, :width]
        if beside:
            sums = [
                [
                    jnp.sum(
                        ref[k * step : (k + 1) * step, width:].astype(jnp.float32)[0:1],
                        keepdims=True,
                    )
                    for k in range(lines)
                ]
                for ref in (half_ref, peer_ref)
            ]
            rest[0][...] = jnp.broadcast_to(tree([tree(x) for x in sums]), (8, 128))

    shapes = [jax.ShapeDtypeStruct((2 * half.shape[0], width), jnp.bfloat16)]
    if beside:
        shapes.append(jax.ShapeDtypeStruct((8, 128), jnp.float32))
    vmem = pl.BlockSpec(memory_space=pltpu.VMEM)
    return pl.pallas_call(
        body,
        in_specs=[pl.BlockSpec(memory_space=pltpu.SMEM), vmem, vmem],
        out_shape=shapes,
        compiler_params=pltpu.CompilerParams(vmem_limit_bytes=4 * 1024 * 1024),
        name="assemble",
    )(index, half, peer)


def normalize(pieces, batch_total):
    values = [p.astype(jnp.float32) for p in pieces]
    mean = sum(jnp.sum(v, axis=0, keepdims=True) for v in values) / batch_total
    var = sum(jnp.sum((v - mean) ** 2, axis=0, keepdims=True) for v in values) / batch_total
    factor = lax.rsqrt(var + variance_floor)
    low = [((v - mean) * factor).astype(jnp.bfloat16) for v in values]
    return mean, factor, lax.optimization_barrier(low)


def gram(low, rows):
    return lax.dot_general(
        low[0][:rows],
        jnp.concatenate(low, axis=0),
        (((1,), (1,)), ((), ())),
        preferred_element_type=jnp.float32,
    )


def local(view_a, view_b):
    rows, cols = view_a.shape
    batch_size = lax.axis_size("batch")
    batch_total = rows * batch_size
    feature_total = cols * lax.axis_size("feat")
    near_a = gather_near(view_a)
    pieces_a = gather_far(near_a)
    near_b = gather_near(view_b)
    pieces_b = gather_far(near_b)
    mean_a, factor_a, low_a = normalize(pieces_a, batch_total)
    own_a = add_terms(scatter_gram(gram(low_a, rows)))
    half_a, peer_a = spread_rows(own_a.astype(jnp.bfloat16))
    (gram_a,) = assemble(half_a, peer_a, batch_total)
    mean_b, factor_b, low_b = normalize(pieces_b, batch_total)
    terms_b = scatter_gram(gram(low_b, rows))
    diag = (
        sum(
            jnp.sum(x.astype(jnp.float32) * y.astype(jnp.float32), axis=0, keepdims=True)
            for x, y in zip(low_a, low_b)
        )
        / batch_total
    )
    pull = 2.0 * (diag - 1.0) - 2.0 * redundancy * diag
    scale = 2.0 * redundancy / batch_total
    sent_b = own_loss(terms_b, own_a, diag, batch_size, batch_total)
    half_b, peer_b = spread_rows(sent_b)
    gram_b, loss_part = assemble(half_b, peer_b, batch_total)
    normed_a = (view_a.astype(jnp.float32) - mean_a) * factor_a
    normed_b = (view_b.astype(jnp.float32) - mean_b) * factor_b

    def backward(gram_other, low, own):
        left = jnp.dot(gram_other, jnp.concatenate(low, axis=0), preferred_element_type=jnp.float32)
        return left * scale + own.astype(jnp.float32) * pull

    dnorm_b = backward(gram_a, low_b, low_a[0])
    dnorm_a = backward(gram_b, low_a, low_b[0])
    stats = jnp.stack(
        [
            jnp.sum(dnorm_a, axis=0),
            jnp.sum(dnorm_a * normed_a, axis=0),
            jnp.sum(dnorm_b, axis=0),
            jnp.sum(dnorm_b * normed_b, axis=0),
            jnp.full((cols,), loss_part[0, 0]),
        ]
    )
    totals = batch_sum(stats)
    loss_value = totals[4, 0] / feature_total
    means = totals[:4] / batch_total
    grad_a = (dnorm_a - means[0] - normed_a * means[1]) * factor_a
    grad_b = (dnorm_b - means[2] - normed_b * means[3]) * factor_b
    return (loss_value, grad_a, grad_b)


def local_any(view_a, view_b):
    rows, cols = view_a.shape
    batch_total = rows * lax.axis_size("batch")
    feature_total = cols * lax.axis_size("feat")
    shift = -rows * lax.axis_index("batch")
    whole_a = jnp.roll(lax.all_gather(view_a, "batch", axis=0, tiled=True), shift, axis=0)
    whole_b = jnp.roll(lax.all_gather(view_b, "batch", axis=0, tiled=True), shift, axis=0)
    mean_a, factor_a, low_a = normalize([whole_a], batch_total)
    mean_b, factor_b, low_b = normalize([whole_b], batch_total)
    gram_a = lax.psum(gram(low_a, rows), "feat")
    gram_b = lax.psum(gram(low_b, rows), "feat")
    own_a = low_a[0][:rows].astype(jnp.float32)
    own_b = low_b[0][:rows].astype(jnp.float32)
    diag = lax.psum(jnp.sum(own_a * own_b, axis=0, keepdims=True), "batch") / batch_total
    pull = 2.0 * (diag - 1.0) - 2.0 * redundancy * diag
    scale = 2.0 * redundancy / batch_total
    ends = lax.psum(jnp.sum((1.0 - diag) ** 2 - redundancy * diag * diag), "feat")
    spread = lax.psum(jnp.sum(gram_a * gram_b), "batch")
    loss = lax.pmax(ends + redundancy * (spread / batch_total**2), ("batch", "feat"))

    def gradient(gram_other, low, own_other, view, mean, factor):
        low_gram = gram_other.astype(jnp.bfloat16)
        dnorm = jnp.dot(low_gram, low[0], preferred_element_type=jnp.float32) * scale + own_other * pull
        normed = (view.astype(jnp.float32) - mean) * factor
        sums = jnp.stack([jnp.sum(dnorm, axis=0), jnp.sum(dnorm * normed, axis=0)])
        means = lax.psum(sums, "batch") / batch_total
        return (dnorm - means[0] - normed * means[1]) * factor

    return (
        loss / feature_total,
        gradient(gram_b, low_a, own_b, view_a, mean_a, factor_a),
        gradient(gram_a, low_b, own_a, view_b, mean_b, factor_b),
    )


def solution(mesh):
    feats = mesh.shape["feat"]
    plain = mesh.shape["batch"] != 4 or feats != 8
    return jax.shard_map(
        local_any if plain else local,
        mesh=mesh,
        in_specs=(P("batch", "feat"), P("batch", "feat")),
        out_specs=(P(), P("batch", "feat"), P("batch", "feat")),
        check_vma=False,
    )
```
